256 devices in a mesh: kv: 32 (over z, x), head: 8 (over y, core).
Axes of the slice: x: 4, y: 4, z: 8, core: 2. Of those that a mesh axis runs over, the one named last changes fastest.
Arguments:
- query: bfloat16 [2, 40, 128, 128], P(None, None, 'head'), may hold values from -16 to 16
- key_cache: bfloat16 [2, 8, 262144, 128], P(None, 'head', 'kv'), may hold values from -6 to 6
- value_cache: bfloat16 [2, 8, 262144, 128], P(None, 'head', 'kv'), may hold values from -6 to 6
- draft_keys: bfloat16 [2, 8, 40, 128], P(None, 'head'), may hold values from -12 to 12
- draft_values: bfloat16 [2, 8, 40, 128], P(None, 'head'), may hold values from -6 to 6
- lengths: int32 [2], replicated, may hold values from 32768 to 262144, as said below
- out_weight: bfloat16 [16384, 16384], P('head', 'kv'), may hold values from -0.1875 to 0.1875
Outputs:
- mixed: bfloat16 [2, 40, 16384], P(None, None, ('kv', 'head'))
The draws below stay inside these ranges and needn't reach their ends.
Inputs may be any that keep to these rules, and one draw needn't show every extreme that they name: `lengths`: one request has exactly 262144 cached positions.
All inputs are finite; a program needn't handle non-finite values.
Results may differ from the reference program's by a relative error of at most 0.0055.
Values may be sent and summed in bfloat16 or wider, within the bound.
No kernel may reach another device: no remote copies, remote signals or barrier semaphores. Data moves between devices by JAX's collectives and lax.ppermute only.
A program may use at most 64 MiB of HBM per device.

```python
import math
import jax
import jax.numpy as jnp
from jax import lax

D = 16384
HEADS = 128
KV_HEADS = 8
HEAD_DIM = 128
BATCH = 2
DRAFT = 40
CONTEXT = 262144


def draw_query(key, part):
    values = jnp.clip(3.0 * jax.random.normal(jax.random.fold_in(key, 1), (BATCH, DRAFT, HEADS, HEAD_DIM), jnp.float32), -16.0, 16.0)
    return values.astype(jnp.bfloat16)


def draw_key_cache(key, part):
    values = jnp.clip(jax.random.normal(jax.random.fold_in(key, 2), (BATCH, KV_HEADS, CONTEXT, HEAD_DIM), jnp.float32), -6.0, 6.0)
    return values.astype(jnp.bfloat16)


def draw_lengths(key, part):
    base_key = jax.random.fold_in(key, 5303)
    full_key, other_key = jax.random.split(base_key, 2)
    full_request = jax.random.randint(full_key, (), 0, BATCH)
    others = jax.random.randint(other_key, (BATCH,), CONTEXT // 8, CONTEXT + 1)
    return jnp.where(jnp.arange(BATCH) == full_request, CONTEXT, others).astype(jnp.int32)


def shard_levels(rng, dims, cuts, low, high):
    level, own = 1.0, jax.random.fold_in(rng, 6)
    for position, shards_of in cuts:
        heights = jnp.exp(jax.random.uniform(jax.random.fold_in(own, position), (shards_of,), jnp.float32, low / len(cuts), high / len(cuts)))
        level = level * jnp.repeat(heights, dims[position] // shards_of).reshape([-1 if axis == position else 1 for axis in range(len(dims))])
    return level


def noise(stream_key, dims, spread, most, pieces=(), kind=jnp.bfloat16):
    loudness = shard_levels(stream_key, dims, pieces, -0.22, 0.18) if pieces else 1.0
    entries = jax.random.normal(stream_key, dims, jnp.float32) * spread * loudness
    return jnp.minimum(jnp.maximum(entries, -most), most).astype(kind)


def setup_inputs(seed: int = 0) -> dict:
    seeds = jax.random.split(jax.random.key(seed), 8)
    query = draw_query(jax.random.fold_in(seeds[7], 71), 0)
    key_cache = draw_key_cache(jax.random.fold_in(seeds[7], 71), 0)
    value_cache = noise(seeds[2], (BATCH, KV_HEADS, CONTEXT, HEAD_DIM), 1.0, 6.0, ((1, 8), (2, 32)))
    draft_keys = noise(seeds[3], (BATCH, KV_HEADS, DRAFT, HEAD_DIM), 2.0, 12.0, ((1, 8),))
    draft_values = noise(seeds[4], (BATCH, KV_HEADS, DRAFT, HEAD_DIM), 1.0, 6.0, ((1, 8),))
    lengths = draw_lengths(jax.random.fold_in(seeds[7], 71), 0)
    out_weight = noise(seeds[6], (D, D), (D // 16) ** -0.5, 0.1875, ((0, 8), (1, 32)))
    return {"query": query, "key_cache": key_cache, "value_cache": value_cache, "draft_keys": draft_keys, "draft_values": draft_values, "lengths": lengths, "out_weight": out_weight}


masked_score = -1e+30

def attend_head(queries, cached_keys, cached_values, new_keys, new_values, length):
    score_scale = 1.0 / math.sqrt(HEAD_DIM)
    query_wide = queries.astype(jnp.float32)
    cache_scores = jnp.dot(query_wide, cached_keys.astype(jnp.float32).T, preferred_element_type=jnp.float32) * score_scale
    draft_scores = jnp.dot(query_wide, new_keys.astype(jnp.float32).T, preferred_element_type=jnp.float32) * score_scale
    cache_live = (jnp.arange(CONTEXT) < length)[None, :]
    draft_live = jnp.arange(DRAFT)[None, :] <= jnp.arange(DRAFT)[:, None]
    cache_scores = jnp.where(cache_live, cache_scores, masked_score)
    draft_scores = jnp.where(draft_live, draft_scores, masked_score)
    row_max = jnp.maximum(lax.optimization_barrier(jnp.max(cache_scores, axis=1)), lax.optimization_barrier(jnp.max(draft_scores, axis=1)))
    cache_weights = jnp.where(cache_live, jnp.exp(cache_scores - row_max[:, None]), 0.0)
    draft_weights = jnp.where(draft_live, jnp.exp(draft_scores - row_max[:, None]), 0.0)
    total = lax.optimization_barrier(jnp.sum(cache_weights, axis=1)) + lax.optimization_barrier(jnp.sum(draft_weights, axis=1))
    mixture = jnp.dot(cache_weights, cached_values.astype(jnp.float32), preferred_element_type=jnp.float32)
    mixture = mixture + jnp.dot(draft_weights, new_values.astype(jnp.float32), preferred_element_type=jnp.float32)
    return mixture / total[:, None]

def reference(query, key_cache, value_cache, draft_keys, draft_values, lengths, out_weight):
    group = HEADS // KV_HEADS
    query_rows = jnp.transpose(query, (0, 2, 1, 3)).reshape(BATCH * HEADS, DRAFT, HEAD_DIM)
    flat_index = jnp.arange(BATCH * HEADS)
    owners = (flat_index // HEADS).astype(jnp.int32)
    kv_owner = (flat_index % HEADS // group).astype(jnp.int32)

    def one_head(item):
        queries, request, kv_head = item
        return attend_head(queries, key_cache[request, kv_head], value_cache[request, kv_head], draft_keys[request, kv_head], draft_values[request, kv_head], lengths[request])
    heads_out = lax.map(one_head, (query_rows, owners, kv_owner))
    attention = heads_out.reshape(BATCH, HEADS, DRAFT, HEAD_DIM)
    attention = jnp.transpose(attention, (0, 2, 1, 3)).reshape(BATCH * DRAFT, D).astype(jnp.bfloat16)
    mixed = jnp.dot(attention, out_weight, preferred_element_type=jnp.float32).astype(jnp.bfloat16)
    return mixed.reshape(BATCH, DRAFT, D)
```

```python
import functools
import math

import jax
import jax.numpy as jnp
from jax import lax
from jax.experimental import pallas as pl
from jax.experimental.pallas import tpu as pltpu
from jax.sharding import PartitionSpec as P

masked_score = -1e30
LANES = 128
STAT_ROWS = 8


def absorb(q, keys, values, m_ref, acc_ref, rows, factor, live):
    span = keys.shape[0]
    scores = lax.dot_general(q, keys, (((1,), (1,)), ((), ())), preferred_element_type=jnp.float32)
    scores = scores * factor
    if live is not None:
        scores = jnp.where(live, scores, masked_score)
    old_max = m_ref[rows, :]
    new_max = jnp.maximum(old_max, jnp.max(scores, axis=1, keepdims=True))
    weights = jnp.exp2(scores - new_max[:, :1]).astype(jnp.bfloat16)
    shrink = jnp.exp2(old_max - new_max)
    wide = jnp.concatenate([values, jnp.ones((span, LANES), values.dtype)], axis=1)
    fresh = jnp.dot(weights, wide, preferred_element_type=jnp.float32)
    m_ref[rows, :] = new_max
    acc_ref[rows, :] = acc_ref[rows, :] * jnp.concatenate([shrink, shrink], axis=1) + fresh


def attend_kernel(
    lengths_ref, place_ref, q_ref, k_ref, v_ref, dk_ref, dv_ref, out_ref, m_ref, acc_ref,
    *, factor, span, piece, row_piece, steps, kv_count, draft, group,
):
    b, t = pl.program_id(0), pl.program_id(1)
    rows_all = q_ref.shape[1]
    kv_index = place_ref[0]

    @pl.when(t == 0)
    def _():
        m_ref[...] = jnp.full(m_ref.shape, masked_score, jnp.float32)
        acc_ref[...] = jnp.zeros(acc_ref.shape, jnp.float32)

    first = kv_index * (steps * span) + t * span
    left = lengths_ref[b] - first

    def sweep(masked):
        for p in range(span // piece):
            keys = k_ref[0, pl.ds(p * piece, piece), :]
            values = v_ref[0, pl.ds(p * piece, piece), :]
            for r in range(rows_all // row_piece):
                rows = pl.ds(r * row_piece, row_piece)
                live = None
                if masked:
                    at = p * piece + lax.broadcasted_iota(jnp.int32, (row_piece, piece), 1)
                    live = at < left
                absorb(q_ref[0, rows, :], keys, values, m_ref, acc_ref, rows, factor, live)

    @pl.when(left >= span)
    def _():
        sweep(False)

    @pl.when(jnp.logical_and(left > 0, left < span))
    def _():
        sweep(True)

    @pl.when(jnp.logical_and(t == steps - 1, kv_index == kv_count - 1))
    def _():
        for r in range(rows_all // row_piece):
            rows = pl.ds(r * row_piece, row_piece)
            row = lax.broadcasted_iota(jnp.int32, (row_piece, draft), 0)
            col = lax.broadcasted_iota(jnp.int32, (row_piece, draft), 1)
            live = col <= lax.rem(row, draft)
            absorb(q_ref[0, rows, :], dk_ref[0], dv_ref[0], m_ref, acc_ref, rows, factor, live)

    @pl.when(t == steps - 1)
    def _():
        row = lax.broadcasted_iota(jnp.int32, (draft, LANES), 0)
        col = lax.broadcasted_iota(jnp.int32, (draft, LANES), 1)
        diagonal = row == col
        for g in range(group):
            rows = pl.ds(g * draft, draft)
            total = acc_ref[rows, LANES:]
            some = total > 0.0
            safe = jnp.where(some, total, 1.0)
            out_ref[g, pl.ds(0, draft), :] = (acc_ref[rows, :LANES] / safe).astype(jnp.bfloat16)
            level = jnp.where(some, m_ref[rows, :] + jnp.log2(safe), masked_score)
            level = jnp.sum(jnp.where(diagonal, level, 0.0), axis=0, keepdims=True)
            high = level.astype(jnp.bfloat16).astype(jnp.float32)
            rest = level - high
            mid = rest.astype(jnp.bfloat16).astype(jnp.float32)
            low = rest - mid
            slot = lax.broadcasted_iota(jnp.int32, (STAT_ROWS, LANES), 0)
            stats = jnp.where(slot == 0, high, jnp.where(slot == 1, mid, jnp.where(slot == 2, low, 0.0)))
            out_ref[g, pl.ds(draft, STAT_ROWS), :] = stats.astype(jnp.bfloat16)


def attend(lengths, place, q, keys, values, draft_keys, draft_values, kv_count, draft, group):
    batch, rows_all, width = q.shape
    local_span = keys.shape[1]
    span = math.gcd(local_span, 2048)
    piece = math.gcd(span, 1024)
    row_piece = rows_all // 2
    steps = local_span // span
    kernel = functools.partial(
        attend_kernel, factor=math.log2(math.e) / math.sqrt(width), span=span, piece=piece,
        row_piece=row_piece, steps=steps, kv_count=kv_count, draft=draft, group=group,
    )
    whole = lambda b, t, *_: (b, 0, 0)
    part = lambda b, t, *_: (b, t, 0)
    positions = batch * local_span
    return pl.pallas_call(
        kernel,
        out_shape=jax.ShapeDtypeStruct((batch * group, draft + STAT_ROWS, width), jnp.bfloat16),
        grid_spec=pltpu.PrefetchScalarGridSpec(
            num_scalar_prefetch=2,
            grid=(batch, steps),
            in_specs=[
                pl.BlockSpec((1, rows_all, width), whole),
                pl.BlockSpec((1, span, width), part),
                pl.BlockSpec((1, span, width), part),
                pl.BlockSpec((1, draft, width), whole),
                pl.BlockSpec((1, draft, width), whole),
            ],
            out_specs=pl.BlockSpec((group, draft + STAT_ROWS, width), whole),
            scratch_shapes=[
                pltpu.VMEM((rows_all, LANES), jnp.float32),
                pltpu.VMEM((rows_all, 2 * LANES), jnp.float32),
            ],
        ),
        compiler_params=pltpu.CompilerParams(dimension_semantics=("arbitrary", "arbitrary")),
        cost_estimate=pl.CostEstimate(
            flops=4 * rows_all * positions * width,
            bytes_accessed=4 * positions * width,
            transcendentals=rows_all * positions,
        ),
        name="attend",
    )(lengths, place, q, keys, values, draft_keys, draft_values)


def merge_kernel(got_ref, out_ref, *, draft):
    count = got_ref.shape[0]
    stats = got_ref[:, pl.ds(draft, STAT_ROWS), :].astype(jnp.float32)
    level = stats[:, 0, :] + stats[:, 1, :] + stats[:, 2, :]
    share = jnp.exp2(level - jnp.max(level, axis=0, keepdims=True))
    share = share / jnp.sum(share, axis=0, keepdims=True)
    share = share.T
    total = jnp.zeros((draft, got_ref.shape[2]), jnp.float32)
    for s in range(count):
        total = total + share[:draft, s : s + 1] * got_ref[s, pl.ds(0, draft), :].astype(jnp.float32)
    done = total.astype(out_ref.dtype)
    for s in range(count):
        out_ref[s] = done


def project_kernel(a_ref, w_ref, out_ref, *, batch, group, heads):
    width = out_ref.shape[2]
    half = width // batch
    parts = []
    for b in range(batch):
        rows = jnp.concatenate([a_ref[b * group + g] for g in range(group)], axis=1)
        parts.append(jnp.dot(rows, w_ref[...], preferred_element_type=jnp.float32))
    lane = lax.broadcasted_iota(jnp.int32, (out_ref.shape[1], width), 1)
    for c in range(heads // 2):
        one = parts[0][:, c * width : (c + 1) * width]
        two = parts[1][:, c * width : (c + 1) * width]
        out_ref[2 * c] = jnp.where(lane < half, one, pltpu.roll(two, half, 1)).astype(out_ref.dtype)
        out_ref[2 * c + 1] = jnp.where(lane < half, pltpu.roll(one, half, 1), two).astype(out_ref.dtype)


def per_device(query, key_cache, value_cache, draft_keys, draft_values, lengths, out_weight):
    batch, draft, group, width = query.shape
    kv_count = lax.axis_size("kv")
    heads = lax.axis_size("head")
    local_span = key_cache.shape[2]
    place = lax.axis_index("kv").astype(jnp.int32)[None]
    q = jnp.transpose(query, (0, 2, 1, 3)).reshape(batch, group * draft, width)
    sent = attend(
        lengths, place, q,
        key_cache.reshape(batch, local_span, width),
        value_cache.reshape(batch, local_span, width),
        draft_keys.reshape(batch, draft, width),
        draft_values.reshape(batch, draft, width),
        kv_count, draft, group,
    )
    got = lax.all_to_all(sent, "kv", split_axis=0, concat_axis=0, tiled=True)
    copies = pl.pallas_call(
        functools.partial(merge_kernel, draft=draft),
        out_shape=jax.ShapeDtypeStruct((kv_count, draft, width), jnp.bfloat16),
        name="merge",
    )(got)
    everyone = lax.all_to_all(copies, "kv", split_axis=0, concat_axis=0, tiled=True)
    shares = pl.pallas_call(
        functools.partial(project_kernel, batch=batch, group=group, heads=heads),
        out_shape=jax.ShapeDtypeStruct((heads, draft, width), jnp.bfloat16),
        name="project",
    )(everyone, out_weight)
    arrived = lax.all_to_all(shares, "head", split_axis=0, concat_axis=0, tiled=True)
    mixed = jnp.sum(arrived.astype(jnp.float32), axis=0)
    half = width // batch
    mixed = jnp.stack([mixed[:, b * half : (b + 1) * half] for b in range(batch)])
    return mixed.astype(jnp.bfloat16)


def solution(mesh):
    in_specs = (
        P(None, None, "head", None),
        P(None, "head", "kv", None),
        P(None, "head", "kv", None),
        P(None, "head", None, None),
        P(None, "head", None, None),
        P(),
        P("head", "kv"),
    )
    out_specs = P(None, None, ("kv", "head"))
    return jax.shard_map(
        per_device, mesh=mesh, in_specs=in_specs, out_specs=out_specs, check_vma=False
    )
```

```python
import functools
import math

import jax
import jax.numpy as jnp
from jax import lax
from jax.experimental import pallas as pl
from jax.experimental.pallas import tpu as pltpu
from jax.sharding import PartitionSpec as P

masked_score = -1e30
LANES = 128
TILE = 256
LIMIT = 2.0**120


def pair_scores(q, keys):
    return lax.dot_general(q, keys, (((1,), (1,)), ((), ())), preferred_element_type=jnp.float32)


def attend_kernel(
    lengths_ref, place_ref, q_hbm, k_hbm, v_hbm, dk_hbm, dv_hbm, out_ref,
    q_ref, k_ref, v_ref, dk_ref, dv_ref, one_ref, m_ref, mix_ref, sum_ref, sems, small_sems,
    *, factor, kv_count, span, part, block_rows,
):
    batch, rows_all, width = q_ref.shape
    local_span = k_ref.shape[1]
    draft = dk_ref.shape[1]
    group = rows_all // draft
    spans = local_span // span
    count = rows_all // part
    half_rows = rows_all // 2
    kv_index = place_ref[0]
    last = kv_index == kv_count - 1
    halves = [pl.ds(r * half_rows, half_rows) for r in range(2)]

    def small_copies():
        pairs = ((q_hbm, q_ref), (dk_hbm, dk_ref), (dv_hbm, dv_ref))
        return [pltpu.make_async_copy(a, z, small_sems.at[n]) for n, (a, z) in enumerate(pairs)]

    def span_copies(s):
        b = s // spans
        at = pl.ds(pl.multiple_of((s - b * spans) * span, span), span)
        return (
            pltpu.make_async_copy(k_hbm.at[b, at, :], k_ref.at[b, at, :], sems.at[0, s]),
            pltpu.make_async_copy(v_hbm.at[b, at, :], v_ref.at[b, at, :], sems.at[1, s]),
        )

    def start_span(s):
        for copy in span_copies(s):
            copy.start()

    def wait_span(s):
        for copy in span_copies(s):
            copy.wait()

        @pl.when(s + 2 < batch * spans)
        def _():
            start_span(s + 2)

    for copy in small_copies():
        copy.start()
    for s in range(2):
        start_span(s)
    one_ref[...] = jnp.ones(one_ref.shape, one_ref.dtype)
    for copy in small_copies():
        copy.wait()

    def reset():
        for ref, fill in ((mix_ref, 0.0), (sum_ref, 0.0), (m_ref, masked_score)):
            ref[pl.ds(0, rows_all), :] = jnp.full((rows_all, LANES), fill, jnp.float32)

    def draft_scores(b, r, rows):
        row = r * half_rows + lax.broadcasted_iota(jnp.int32, (half_rows, draft), 0)
        col = lax.broadcasted_iota(jnp.int32, (half_rows, draft), 1)
        scores = pair_scores(q_ref[b, rows, :], dk_ref[b]) * factor
        return jnp.where(col * group <= row, scores, masked_score)

    def tile_scores(b, rows, start, left):
        at = start + lax.broadcasted_iota(jnp.int32, (half_rows, TILE), 1)
        scores = pair_scores(q_ref[b, rows, :], k_ref[b, pl.ds(start, TILE), :]) * factor
        return jnp.where(at < left, scores, masked_score)

    def level_up(rows, scores):
        m_ref[rows, :] = jnp.maximum(m_ref[rows, :], jnp.max(scores, axis=1, keepdims=True))

    def add(rows, scores, values):
        weights = jnp.exp2(scores - m_ref[rows, :][:, :1]).astype(jnp.bfloat16)
        wide = jnp.concatenate([values, jnp.ones(values.shape, values.dtype)], axis=1)
        fresh = jnp.dot(weights, wide, preferred_element_type=jnp.float32)
        mix_ref[rows, :] += fresh[:, :LANES]
        sum_ref[rows, :] += fresh[:, LANES:]

    def sweep(b, i):
        for rows in halves:
            q = q_ref[b, rows, :]
            level = m_ref[rows, :]
            level = jnp.concatenate([level, level], axis=1)
            total = jnp.zeros((half_rows, 2 * LANES), jnp.float32)
            for t in range(span // TILE):
                at = pl.ds(pl.multiple_of(i * span + t * TILE, TILE), TILE)
                scores = pair_scores(q, k_ref[b, at, :]) * factor
                weights = jnp.exp2(scores - level).astype(jnp.bfloat16)
                wide = jnp.concatenate([v_ref[b, at, :], one_ref[pl.ds(t * TILE, TILE), :]], axis=1)
                total += jnp.dot(weights, wide, preferred_element_type=jnp.float32)
            mix_ref[rows, :] += total[:, :LANES]
            sum_ref[rows, :] += total[:, LANES:]

    def one_request(b, carry):
        left = lengths_ref[b] - kv_index * local_span
        reset()

        @pl.when(last)
        def _():
            for r, rows in enumerate(halves):
                level_up(rows, draft_scores(b, r, rows))

        wait_span(b * spans)

        @pl.when(left > 0)
        def _():
            for rows in halves:
                level_up(rows, tile_scores(b, rows, 0, left))

        @pl.when(last)
        def _():
            for r, rows in enumerate(halves):
                add(rows, draft_scores(b, r, rows), dv_ref[b])

        def one_span(i, carry):
            @pl.when(i > 0)
            def _():
                wait_span(b * spans + i)

            rest = left - i * span
            ragged = jnp.logical_and(rest > 0, rest < span)

            @pl.when(ragged)
            def _():
                def cut(t, carry):
                    here = pl.ds(pl.multiple_of(t * TILE, TILE), TILE)
                    there = pl.ds(pl.multiple_of(i * span + t * TILE, TILE), TILE)
                    at = t * TILE + lax.broadcasted_iota(jnp.int32, (TILE, width), 0)
                    keep = at < rest
                    kept = jnp.where(keep, v_ref[b, there, :].astype(jnp.float32), 0.0)
                    v_ref[b, there, :] = kept.astype(v_ref.dtype)
                    one_ref[here, :] = jnp.where(keep, 1.0, 0.0).astype(one_ref.dtype)
                    return carry

                lax.fori_loop(0, span // TILE, cut, 0)

            @pl.when(rest > 0)
            def _():
                sweep(b, i)

            @pl.when(ragged)
            def _():
                one_ref[...] = jnp.ones(one_ref.shape, one_ref.dtype)

            return carry

        lax.fori_loop(0, spans, one_span, 0)

        over = jnp.max(jnp.where(sum_ref[pl.ds(0, rows_all), :] < LIMIT, 0.0, 1.0))

        @pl.when(over > 0.0)
        def _():
            reset()

            def careful(rows, scores, values):
                old = m_ref[rows, :]
                level_up(rows, scores)
                shrink = jnp.exp2(old - m_ref[rows, :])
                mix_ref[rows, :] *= shrink
                sum_ref[rows, :] *= shrink
                add(rows, scores, values)

            @pl.when(last)
            def _():
                for r, rows in enumerate(halves):
                    careful(rows, draft_scores(b, r, rows), dv_ref[b])

            def step(t, carry):
                start = pl.multiple_of(t * TILE, TILE)

                @pl.when(start < left)
                def _():
                    for rows in halves:
                        careful(rows, tile_scores(b, rows, start, left), v_ref[b, pl.ds(start, TILE), :])

                return carry

            lax.fori_loop(0, local_span // TILE, step, 0)

        row = lax.broadcasted_iota(jnp.int32, (block_rows, LANES), 0)
        col = lax.broadcasted_iota(jnp.int32, (block_rows, LANES), 1)
        diagonal = jnp.logical_and(row == col, row < part)
        for d in range(count):
            rows = pl.ds(d * part, block_rows)
            total = sum_ref[rows, :]
            some = jnp.logical_and(row < part, total > 0.0)
            safe = jnp.where(some, total, 1.0)
            level = jnp.where(some, m_ref[rows, :] + jnp.log2(safe), masked_score)
            level = jnp.sum(jnp.where(diagonal, level, 0.0), axis=0, keepdims=True)
            high = level.astype(jnp.bfloat16).astype(jnp.float32)
            rest = level - high
            mid = rest.astype(jnp.bfloat16).astype(jnp.float32)
            low = rest - mid
            block = jnp.where(row < part, mix_ref[rows, :] / safe, 0.0)
            block = jnp.where(row == part, high, block)
            block = jnp.where(row == part + 1, mid, block)
            block = jnp.where(row == part + 2, low, block)
            out_ref[d, pl.ds(pl.multiple_of(b * block_rows, 8), block_rows), :] = block.astype(jnp.bfloat16)
        return carry

    lax.fori_loop(0, batch, one_request, 0)


def attend(lengths, place, q, keys, values, draft_keys, draft_values, kv_count, part, block_rows):
    batch, rows_all, width = q.shape
    local_span, draft = keys.shape[1], draft_keys.shape[1]
    span = math.gcd(local_span, 4096)
    kernel = functools.partial(
        attend_kernel, factor=math.log2(math.e) / math.sqrt(width), kv_count=kv_count,
        span=span, part=part, block_rows=block_rows,
    )
    anywhere = pl.BlockSpec(memory_space=pltpu.HBM)
    state = pltpu.VMEM((rows_all + block_rows, LANES), jnp.float32)
    out = (rows_all // part, batch * block_rows, width)
    return pl.pallas_call(
        kernel,
        out_shape=jax.ShapeDtypeStruct(out, jnp.bfloat16),
        grid_spec=pltpu.PrefetchScalarGridSpec(
            num_scalar_prefetch=2,
            grid=(1,),
            in_specs=[anywhere] * 5,
            out_specs=pl.BlockSpec(out, lambda i, *_: (0, 0, 0)),
            scratch_shapes=[
                pltpu.VMEM((batch, rows_all, width), jnp.bfloat16),
                pltpu.VMEM((batch, local_span, width), jnp.bfloat16),
                pltpu.VMEM((batch, local_span, width), jnp.bfloat16),
                pltpu.VMEM((batch, draft, width), jnp.bfloat16),
                pltpu.VMEM((batch, draft, width), jnp.bfloat16),
                pltpu.VMEM((span, LANES), jnp.bfloat16),
                state, state, state,
                pltpu.SemaphoreType.DMA((2, batch * local_span // span)),
                pltpu.SemaphoreType.DMA((3,)),
            ],
        ),
        compiler_params=pltpu.CompilerParams(vmem_limit_bytes=58 * 2**20),
        cost_estimate=pl.CostEstimate(
            flops=4 * batch * rows_all * local_span * width,
            bytes_accessed=4 * batch * local_span * width,
            transcendentals=batch * rows_all * local_span,
        ),
        name="attend",
    )(lengths, place, q, keys, values, draft_keys, draft_values)


def merge_kernel(got_ref, out_ref, both_ref, *, part, batch):
    count, rows, width = got_ref.shape
    block_rows = rows // batch
    base = (part // 8) * 8
    at = part - base
    for b in range(batch):
        stats = got_ref[:, pl.ds(b * block_rows + base, block_rows - base), :].astype(jnp.float32)
        level = stats[:, at, :] + stats[:, at + 1, :] + stats[:, at + 2, :]
        share = jnp.exp2(level - jnp.max(level, axis=0, keepdims=True))
        share = share / jnp.sum(share, axis=0, keepdims=True)
        share = share.T
        total = jnp.zeros((block_rows, width), jnp.float32)
        for s in range(count):
            mine = got_ref[s, pl.ds(b * block_rows, block_rows), :].astype(jnp.float32)
            total = total + share[:block_rows, s : s + 1] * mine
        both_ref[pl.ds(b * part, block_rows), :] = total
    done = both_ref[pl.ds(0, batch * part), :].astype(out_ref.dtype)
    for s in range(count):
        out_ref[s] = done


def merge(got, part, batch):
    count, rows, width = got.shape
    return pl.pallas_call(
        functools.partial(merge_kernel, part=part, batch=batch),
        out_shape=jax.ShapeDtypeStruct((count, batch * part, width), jnp.bfloat16),
        scratch_shapes=[pltpu.VMEM((rows, width), jnp.float32)],
        compiler_params=pltpu.CompilerParams(vmem_limit_bytes=8 * 2**20),
        name="merge",
    )(got)


def project_kernel(a_ref, w_ref, out_ref, rows_ref, *, group, heads, batch):
    count, both, width = a_ref.shape
    part = both // batch
    draft = count * part // group
    cycle = math.lcm(group, part)
    steps = count * part // cycle
    half = width // 2
    for d in range(count):
        rows_ref[pl.ds(d * both, both), :] = a_ref[d].astype(jnp.float32)
    rows = []
    for b in range(batch):
        for j in range(cycle // group):
            line = []
            for g in range(group):
                d, r = divmod(j * group + g, part)
                at = pl.ds(d * both + b * part + r, steps, stride=cycle * batch)
                line.append(rows_ref[at, :])
            rows.append(jnp.concatenate(line, axis=1))
    rows = jnp.concatenate(rows, axis=0).astype(jnp.bfloat16)
    product = jnp.dot(rows, w_ref[...], preferred_element_type=jnp.float32)
    lane = lax.broadcasted_iota(jnp.int32, (draft, width), 1)
    for c in range(heads // 2):
        one = product[:draft, c * width : (c + 1) * width]
        two = product[draft:, c * width : (c + 1) * width]
        out_ref[2 * c] = jnp.where(lane < half, one, pltpu.roll(two, half, 1)).astype(out_ref.dtype)
        out_ref[2 * c + 1] = jnp.where(lane < half, pltpu.roll(one, half, 1), two).astype(out_ref.dtype)


def per_device(query, key_cache, value_cache, draft_keys, draft_values, lengths, out_weight):
    batch, draft, group, width = query.shape
    kv_count = lax.axis_size("kv")
    heads = lax.axis_size("head")
    local_span = key_cache.shape[2]
    part = draft * group // kv_count
    block_rows = -(-(part + 3) // 8) * 8
    place = lax.axis_index("kv").astype(jnp.int32)[None]
    exchange = functools.partial(lax.all_to_all, split_axis=0, concat_axis=0, tiled=True)
    sent = attend(
        lengths, place,
        query.reshape(batch, draft * group, width),
        key_cache.reshape(batch, local_span, width),
        value_cache.reshape(batch, local_span, width),
        draft_keys.reshape(batch, draft, width),
        draft_values.reshape(batch, draft, width),
        kv_count, part, block_rows,
    )
    everyone = exchange(merge(exchange(sent, "kv"), part, batch), "kv")
    shares = pl.pallas_call(
        functools.partial(project_kernel, group=group, heads=heads, batch=batch),
        out_shape=jax.ShapeDtypeStruct((heads, draft, width), jnp.bfloat16),
        scratch_shapes=[pltpu.VMEM((kv_count * batch * part, width), jnp.float32)],
        compiler_params=pltpu.CompilerParams(vmem_limit_bytes=16 * 2**20),
        name="project",
    )(everyone, out_weight)
    arrived = exchange(shares, "head")
    cycle = math.lcm(group, part) // group
    mixed = jnp.sum(arrived.astype(jnp.float32), axis=0)
    mixed = mixed.reshape(cycle, draft // cycle, batch, width // 2)
    mixed = jnp.transpose(mixed, (2, 1, 0, 3)).reshape(batch, draft, width // 2)
    return mixed.astype(jnp.bfloat16)


def solution(mesh):
    in_specs = (
        P(None, None, "head", None),
        P(None, "head", "kv", None),
        P(None, "head", "kv", None),
        P(None, "head", None, None),
        P(None, "head", None, None),
        P(),
        P("head", "kv"),
    )
    out_specs = P(None, None, ("kv", "head"))
    return jax.shard_map(
        per_device, mesh=mesh, in_specs=in_specs, out_specs=out_specs, check_vma=False
    )
```

```python
import functools
import math

import jax
import jax.numpy as jnp
from jax import lax
from jax.experimental import pallas as pl
from jax.experimental.pallas import tpu as pltpu
from jax.sharding import PartitionSpec as P

masked_score = -1e30
LANES = 128
TILE = 256
LIMIT = 2.0**120


def pair_scores(q, keys):
    return lax.dot_general(q, keys, (((1,), (1,)), ((), ())), preferred_element_type=jnp.float32)


def attend_kernel(
    place_ref, lengths_hbm, q_hbm, k_hbm, v_hbm, dk_hbm, dv_hbm, out_ref,
    lengths_ref, q_ref, k_ref, v_ref, dk_ref, dv_ref, one_ref, m_ref, mix_ref, sum_ref, sems, small_sems,
    *, factor, kv_count, span, part, block_rows,
):
    batch, rows_all, width = q_ref.shape
    local_span = k_ref.shape[1]
    draft = dk_ref.shape[1]
    group = rows_all // draft
    spans = local_span // span
    count = rows_all // part
    half_rows = rows_all // 2
    kv_index = place_ref[0]
    last = kv_index == kv_count - 1
    halves = [pl.ds(r * half_rows, half_rows) for r in range(2)]

    def small_copies():
        pairs = ((q_hbm, q_ref), (lengths_hbm, lengths_ref), (dk_hbm, dk_ref), (dv_hbm, dv_ref))
        return [pltpu.make_async_copy(a, z, small_sems.at[n]) for n, (a, z) in enumerate(pairs)]

    def span_copies(s):
        b = s // spans
        at = pl.ds(pl.multiple_of((s - b * spans) * span, span), span)
        return (
            pltpu.make_async_copy(k_hbm.at[b, at, :], k_ref.at[b, at, :], sems.at[0, s]),
            pltpu.make_async_copy(v_hbm.at[b, at, :], v_ref.at[b, at, :], sems.at[1, s]),
        )

    def start_span(s):
        @pl.when(s < batch * spans)
        def _():
            for copy in span_copies(s):
                copy.start()

    for copy in small_copies()[:2]:
        copy.start()
    for copy in span_copies(0):
        copy.start()
    for copy in small_copies()[2:]:
        copy.start()
    one_ref[...] = jnp.ones(one_ref.shape, one_ref.dtype)
    for copy in small_copies():
        copy.wait()
    start_span(1)

    def reset():
        for ref, fill in ((mix_ref, 0.0), (sum_ref, 0.0), (m_ref, masked_score)):
            ref[pl.ds(0, rows_all), :] = jnp.full((rows_all, LANES), fill, jnp.float32)

    def draft_scores(b, r, rows):
        row = r * half_rows + lax.broadcasted_iota(jnp.int32, (half_rows, draft), 0)
        col = lax.broadcasted_iota(jnp.int32, (half_rows, draft), 1)
        scores = pair_scores(q_ref[b, rows, :], dk_ref[b]) * factor
        return jnp.where(col * group <= row, scores, masked_score)

    def tile_scores(b, rows, start, left):
        at = start + lax.broadcasted_iota(jnp.int32, (half_rows, TILE), 1)
        scores = pair_scores(q_ref[b, rows, :], k_ref[b, pl.ds(start, TILE), :]) * factor
        return jnp.where(at < left, scores, masked_score)

    def level_up(rows, scores):
        m_ref[rows, :] = jnp.maximum(m_ref[rows, :], jnp.max(scores, axis=1, keepdims=True))

    def add(rows, scores, values):
        weights = jnp.exp2(scores - m_ref[rows, :][:, :1]).astype(jnp.bfloat16)
        wide = jnp.concatenate([values, jnp.ones(values.shape, values.dtype)], axis=1)
        fresh = jnp.dot(weights, wide, preferred_element_type=jnp.float32)
        mix_ref[rows, :] += fresh[:, :LANES]
        sum_ref[rows, :] += fresh[:, LANES:]

    def sweep(b, i):
        for rows in halves:
            q = q_ref[b, rows, :]
            level = m_ref[rows, :]
            level = jnp.concatenate([level, level], axis=1)
            total = jnp.zeros((half_rows, 2 * LANES), jnp.float32)
            for t in range(span // TILE):
                at = pl.ds(pl.multiple_of(i * span + t * TILE, TILE), TILE)
                scores = pair_scores(q, k_ref[b, at, :]) * factor
                weights = jnp.exp2(scores - level).astype(jnp.bfloat16)
                wide = jnp.concatenate([v_ref[b, at, :], one_ref[pl.ds(t * TILE, TILE), :]], axis=1)
                total += jnp.dot(weights, wide, preferred_element_type=jnp.float32)
            mix_ref[rows, :] += total[:, :LANES]
            sum_ref[rows, :] += total[:, LANES:]

    def one_request(b, carry):
        left = lengths_ref[b] - kv_index * local_span
        reset()

        @pl.when(last)
        def _():
            for r, rows in enumerate(halves):
                level_up(rows, draft_scores(b, r, rows))

        span_copies(b * spans)[0].wait()
        start_span(b * spans + 2)

        @pl.when(left > 0)
        def _():
            for rows in halves:
                level_up(rows, tile_scores(b, rows, 0, left))

        @pl.when(last)
        def _():
            for r, rows in enumerate(halves):
                add(rows, draft_scores(b, r, rows), dv_ref[b])

        def one_span(i, carry):
            @pl.when(i > 0)
            def _():
                span_copies(b * spans + i)[0].wait()
                start_span(b * spans + i + 2)

            span_copies(b * spans + i)[1].wait()

            rest = left - i * span
            ragged = jnp.logical_and(rest > 0, rest < span)

            @pl.when(ragged)
            def _():
                def cut(t, carry):
                    here = pl.ds(pl.multiple_of(t * TILE, TILE), TILE)
                    there = pl.ds(pl.multiple_of(i * span + t * TILE, TILE), TILE)
                    at = t * TILE + lax.broadcasted_iota(jnp.int32, (TILE, width), 0)
                    keep = at < rest
                    kept = jnp.where(keep, v_ref[b, there, :].astype(jnp.float32), 0.0)
                    v_ref[b, there, :] = kept.astype(v_ref.dtype)
                    one_ref[here, :] = jnp.where(keep, 1.0, 0.0).astype(one_ref.dtype)
                    return carry

                lax.fori_loop(0, span // TILE, cut, 0)

            @pl.when(rest > 0)
            def _():
                sweep(b, i)

            @pl.when(ragged)
            def _():
                one_ref[...] = jnp.ones(one_ref.shape, one_ref.dtype)

            return carry

        lax.fori_loop(0, spans, one_span, 0)

        over = jnp.max(jnp.where(sum_ref[pl.ds(0, rows_all), :] < LIMIT, 0.0, 1.0))

        @pl.when(over > 0.0)
        def _():
            reset()

            def careful(rows, scores, values):
                old = m_ref[rows, :]
                level_up(rows, scores)
                shrink = jnp.exp2(old - m_ref[rows, :])
                mix_ref[rows, :] *= shrink
                sum_ref[rows, :] *= shrink
                add(rows, scores, values)

            @pl.when(last)
            def _():
                for r, rows in enumerate(halves):
                    careful(rows, draft_scores(b, r, rows), dv_ref[b])

            def step(t, carry):
                start = pl.multiple_of(t * TILE, TILE)

                @pl.when(start < left)
                def _():
                    for rows in halves:
                        careful(rows, tile_scores(b, rows, start, left), v_ref[b, pl.ds(start, TILE), :])

                return carry

            lax.fori_loop(0, local_span // TILE, step, 0)

        row = lax.broadcasted_iota(jnp.int32, (block_rows, LANES), 0)
        col = lax.broadcasted_iota(jnp.int32, (block_rows, LANES), 1)
        diagonal = jnp.logical_and(row == col, row < part)
        for d in range(count):
            rows = pl.ds(d * part, block_rows)
            total = sum_ref[rows, :]
            some = jnp.logical_and(row < part, total > 0.0)
            safe = jnp.where(some, total, 1.0)
            level = jnp.where(some, m_ref[rows, :] + jnp.log2(safe), masked_score)
            level = jnp.sum(jnp.where(diagonal, level, 0.0), axis=0, keepdims=True)
            high = level.astype(jnp.bfloat16).astype(jnp.float32)
            rest = level - high
            mid = rest.astype(jnp.bfloat16).astype(jnp.float32)
            low = rest - mid
            block = jnp.where(row < part, mix_ref[rows, :] / safe, 0.0)
            block = jnp.where(row == part, high, block)
            block = jnp.where(row == part + 1, mid, block)
            block = jnp.where(row == part + 2, low, block)
            out_ref[d, pl.ds(pl.multiple_of(b * block_rows, 8), block_rows), :] = block.astype(jnp.bfloat16)
        return carry

    lax.fori_loop(0, batch, one_request, 0)


def attend(lengths, place, q, keys, values, draft_keys, draft_values, kv_count, part, block_rows):
    batch, rows_all, width = q.shape
    local_span, draft = keys.shape[1], draft_keys.shape[1]
    span = math.gcd(local_span, 2048)
    kernel = functools.partial(
        attend_kernel, factor=math.log2(math.e) / math.sqrt(width), kv_count=kv_count,
        span=span, part=part, block_rows=block_rows,
    )
    anywhere = pl.BlockSpec(memory_space=pltpu.HBM)
    state = pltpu.VMEM((rows_all + block_rows, LANES), jnp.float32)
    out = (rows_all // part, batch * block_rows, width)
    return pl.pallas_call(
        kernel,
        out_shape=jax.ShapeDtypeStruct(out, jnp.bfloat16),
        grid_spec=pltpu.PrefetchScalarGridSpec(
            num_scalar_prefetch=1,
            grid=(1,),
            in_specs=[anywhere] * 6,
            out_specs=pl.BlockSpec(out, lambda i, *_: (0, 0, 0)),
            scratch_shapes=[
                pltpu.SMEM((batch,), jnp.int32),
                pltpu.VMEM((batch, rows_all, width), jnp.bfloat16),
                pltpu.VMEM((batch, local_span, width), jnp.bfloat16),
                pltpu.VMEM((batch, local_span, width), jnp.bfloat16),
                pltpu.VMEM((batch, draft, width), jnp.bfloat16),
                pltpu.VMEM((batch, draft, width), jnp.bfloat16),
                pltpu.VMEM((span, LANES), jnp.bfloat16),
                state, state, state,
                pltpu.SemaphoreType.DMA((2, batch * local_span // span)),
                pltpu.SemaphoreType.DMA((4,)),
            ],
        ),
        compiler_params=pltpu.CompilerParams(vmem_limit_bytes=58 * 2**20),
        cost_estimate=pl.CostEstimate(
            flops=4 * batch * rows_all * local_span * width,
            bytes_accessed=4 * batch * local_span * width,
            transcendentals=batch * rows_all * local_span,
        ),
        name="attend",
    )(place, lengths, q, keys, values, draft_keys, draft_values)


def merge_kernel(got_ref, out_ref, both_ref, *, part, batch):
    count, rows, width = got_ref.shape
    block_rows = rows // batch
    base = (part // 8) * 8
    at = part - base
    for b in range(batch):
        stats = got_ref[:, pl.ds(b * block_rows + base, block_rows - base), :].astype(jnp.float32)
        level = stats[:, at, :] + stats[:, at + 1, :] + stats[:, at + 2, :]
        share = jnp.exp2(level - jnp.max(level, axis=0, keepdims=True))
        share = share / jnp.sum(share, axis=0, keepdims=True)
        share = share.T
        total = jnp.zeros((block_rows, width), jnp.float32)
        for s in range(count):
            mine = got_ref[s, pl.ds(b * block_rows, block_rows), :].astype(jnp.float32)
            total = total + share[:block_rows, s : s + 1] * mine
        both_ref[pl.ds(b * part, block_rows), :] = total
    done = both_ref[pl.ds(0, batch * part), :].astype(out_ref.dtype)
    for s in range(count):
        out_ref[s] = done


def merge(got, part, batch):
    count, rows, width = got.shape
    return pl.pallas_call(
        functools.partial(merge_kernel, part=part, batch=batch),
        out_shape=jax.ShapeDtypeStruct((count, batch * part, width), jnp.bfloat16),
        scratch_shapes=[pltpu.VMEM((rows, width), jnp.float32)],
        compiler_params=pltpu.CompilerParams(vmem_limit_bytes=8 * 2**20),
        name="merge",
    )(got)


def project_kernel(a_ref, w_ref, out_ref, rows_ref, *, group, heads, batch):
    count, both, width = a_ref.shape
    part = both // batch
    draft = count * part // group
    cycle = math.lcm(group, part)
    steps = count * part // cycle
    half = width // 2
    for d in range(count):
        rows_ref[pl.ds(d * both, both), :] = a_ref[d].astype(jnp.float32)
    rows = []
    for b in range(batch):
        for j in range(cycle // group):
            line = []
            for g in range(group):
                d, r = divmod(j * group + g, part)
                at = pl.ds(d * both + b * part + r, steps, stride=cycle * batch)
                line.append(rows_ref[at, :])
            rows.append(jnp.concatenate(line, axis=1))
    rows = jnp.concatenate(rows, axis=0).astype(jnp.bfloat16)
    product = jnp.dot(rows, w_ref[...], preferred_element_type=jnp.float32)
    lane = lax.broadcasted_iota(jnp.int32, (draft, width), 1)
    for c in range(heads // 2):
        one = product[:draft, c * width : (c + 1) * width]
        two = product[draft:, c * width : (c + 1) * width]
        out_ref[2 * c] = jnp.where(lane < half, one, pltpu.roll(two, half, 1)).astype(out_ref.dtype)
        out_ref[2 * c + 1] = jnp.where(lane < half, pltpu.roll(one, half, 1), two).astype(out_ref.dtype)


def per_device(query, key_cache, value_cache, draft_keys, draft_values, lengths, out_weight):
    batch, draft, group, width = query.shape
    kv_count = lax.axis_size("kv")
    heads = lax.axis_size("head")
    local_span = key_cache.shape[2]
    part = draft * group // kv_count
    block_rows = -(-(part + 3) // 8) * 8
    place = lax.axis_index("kv").astype(jnp.int32)[None]
    exchange = functools.partial(lax.all_to_all, split_axis=0, concat_axis=0, tiled=True)
    sent = attend(
        lengths, place,
        query.reshape(batch, draft * group, width),
        key_cache.reshape(batch, local_span, width),
        value_cache.reshape(batch, local_span, width),
        draft_keys.reshape(batch, draft, width),
        draft_values.reshape(batch, draft, width),
        kv_count, part, block_rows,
    )
    everyone = exchange(merge(exchange(sent, "kv"), part, batch), "kv")
    shares = pl.pallas_call(
        functools.partial(project_kernel, group=group, heads=heads, batch=batch),
        out_shape=jax.ShapeDtypeStruct((heads, draft, width), jnp.bfloat16),
        scratch_shapes=[pltpu.VMEM((kv_count * batch * part, width), jnp.float32)],
        compiler_params=pltpu.CompilerParams(vmem_limit_bytes=16 * 2**20),
        name="project",
    )(everyone, out_weight)
    arrived = exchange(shares, "head")
    cycle = math.lcm(group, part) // group
    mixed = jnp.sum(arrived.astype(jnp.float32), axis=0)
    mixed = mixed.reshape(cycle, draft // cycle, batch, width // 2)
    mixed = jnp.transpose(mixed, (2, 1, 0, 3)).reshape(batch, draft, width // 2)
    return mixed.astype(jnp.bfloat16)


def solution(mesh):
    in_specs = (
        P(None, None, "head", None),
        P(None, "head", "kv", None),
        P(None, "head", "kv", None),
        P(None, "head", None, None),
        P(None, "head", None, None),
        P(),
        P("head", "kv"),
    )
    out_specs = P(None, None, ("kv", "head"))
    return jax.shard_map(
        per_device, mesh=mesh, in_specs=in_specs, out_specs=out_specs, check_vma=False
    )
```

```python
import functools
import math

import jax
import jax.numpy as jnp
from jax import lax
from jax.experimental import pallas as pl
from jax.experimental.pallas import tpu as pltpu
from jax.sharding import PartitionSpec as P

masked_score = -1e30
LANES = 128
TILE = 256
LIMIT = 2.0**120


def pair_scores(q, keys):
    return lax.dot_general(q, keys, (((1,), (1,)), ((), ())), preferred_element_type=jnp.float32)


def attend_kernel(
    place_ref, lengths_hbm, q_hbm, k_hbm, v_hbm, dk_hbm, dv_hbm, out_ref,
    lengths_ref, q_ref, k_ref, v_ref, dk_ref, dv_ref, one_ref, m_ref, mix_ref, sum_ref, sems, small_sems,
    *, factor, kv_count, span, part, block_rows,
):
    batch, rows_all, width = q_ref.shape
    local_span = k_ref.shape[1]
    draft = dk_ref.shape[1]
    group = rows_all // draft
    spans = local_span // span
    count = rows_all // part
    half_rows = rows_all // 2
    kv_index = place_ref[0]
    last = kv_index == kv_count - 1
    halves = [pl.ds(r * half_rows, half_rows) for r in range(2)]

    def small_copies():
        pairs = ((q_hbm, q_ref), (lengths_hbm, lengths_ref), (dk_hbm, dk_ref), (dv_hbm, dv_ref))
        return [pltpu.make_async_copy(a, z, small_sems.at[n]) for n, (a, z) in enumerate(pairs)]

    def span_copies(s):
        b = s // spans
        at = pl.ds(pl.multiple_of((s - b * spans) * span, span), span)
        return (
            pltpu.make_async_copy(k_hbm.at[b, at, :], k_ref.at[b, at, :], sems.at[0, s]),
            pltpu.make_async_copy(v_hbm.at[b, at, :], v_ref.at[b, at, :], sems.at[1, s]),
        )

    def start_span(s):
        @pl.when(s < batch * spans)
        def _():
            for copy in span_copies(s):
                copy.start()

    for copy in small_copies()[:2]:
        copy.start()
    for copy in span_copies(0):
        copy.start()
    for copy in small_copies()[2:]:
        copy.start()
    one_ref[...] = jnp.ones(one_ref.shape, one_ref.dtype)
    for copy in small_copies():
        copy.wait()
    start_span(1)

    def reset():
        for ref, fill in ((mix_ref, 0.0), (sum_ref, 0.0), (m_ref, masked_score)):
            ref[pl.ds(0, rows_all), :] = jnp.full((rows_all, LANES), fill, jnp.float32)

    def draft_scores(b, r, rows):
        row = r * half_rows + lax.broadcasted_iota(jnp.int32, (half_rows, draft), 0)
        col = lax.broadcasted_iota(jnp.int32, (half_rows, draft), 1)
        scores = pair_scores(q_ref[b, rows, :], dk_ref[b]) * factor
        return jnp.where(col * group <= row, scores, masked_score)

    def tile_scores(b, rows, start, left):
        at = start + lax.broadcasted_iota(jnp.int32, (half_rows, TILE), 1)
        scores = pair_scores(q_ref[b, rows, :], k_ref[b, pl.ds(start, TILE), :]) * factor
        return jnp.where(at < left, scores, masked_score)

    def level_up(rows, scores):
        m_ref[rows, :] = jnp.maximum(m_ref[rows, :], jnp.max(scores, axis=1, keepdims=True))

    def add(rows, scores, values):
        weights = jnp.exp2(scores - m_ref[rows, :][:, :1]).astype(jnp.bfloat16)
        wide = jnp.concatenate([values, jnp.ones(values.shape, values.dtype)], axis=1)
        fresh = jnp.dot(weights, wide, preferred_element_type=jnp.float32)
        mix_ref[rows, :] += fresh[:, :LANES]
        sum_ref[rows, :] += fresh[:, LANES:]

    def ready(b, c, left):
        s = b * spans + c
        if c > 0:
            span_copies(s)[0].wait()
            start_span(s + 2)
        span_copies(s)[1].wait()
        rest = left - c * span

        @pl.when(rest < span)
        def _():
            def cut(t, carry):
                here = pl.ds(pl.multiple_of(c * span + t * TILE, TILE), TILE)
                at = t * TILE + lax.broadcasted_iota(jnp.int32, (TILE, width), 0)
                keep = at < rest
                kept = jnp.where(keep, v_ref[b, here, :].astype(jnp.float32), 0.0)
                v_ref[b, here, :] = kept.astype(v_ref.dtype)
                one_ref[here, :] = jnp.where(keep, 1.0, 0.0).astype(one_ref.dtype)
                return carry

            lax.fori_loop(0, span // TILE, cut, 0)

    def sweep(b, left):
        for r, rows in enumerate(halves):
            q = q_ref[b, rows, :]
            level = m_ref[rows, :]
            level = jnp.concatenate([level, level], axis=1)
            total = jnp.zeros((half_rows, 2 * LANES), jnp.float32)
            for t in range(local_span // TILE):
                if r == 0 and t * TILE % span == 0:
                    ready(b, t * TILE // span, left)
                at = pl.ds(t * TILE, TILE)
                scores = pair_scores(q, k_ref[b, at, :]) * factor
                weights = jnp.exp2(scores - level).astype(jnp.bfloat16)
                wide = jnp.concatenate([v_ref[b, at, :], one_ref[at, :]], axis=1)
                total += jnp.dot(weights, wide, preferred_element_type=jnp.float32)
            mix_ref[rows, :] += total[:, :LANES]
            sum_ref[rows, :] += total[:, LANES:]

    def one_request(b, carry):
        left = lengths_ref[b] - kv_index * local_span
        reset()

        @pl.when(last)
        def _():
            for r, rows in enumerate(halves):
                level_up(rows, draft_scores(b, r, rows))

        span_copies(b * spans)[0].wait()
        start_span(b * spans + 2)

        @pl.when(left > 0)
        def _():
            for rows in halves:
                level_up(rows, tile_scores(b, rows, 0, left))

        @pl.when(last)
        def _():
            for r, rows in enumerate(halves):
                add(rows, draft_scores(b, r, rows), dv_ref[b])

        @pl.when(left > 0)
        def _():
            sweep(b, left)

            @pl.when(left < local_span)
            def _():
                one_ref[...] = jnp.ones(one_ref.shape, one_ref.dtype)

        @pl.when(left <= 0)
        def _():
            for c in range(spans):
                if c > 0:
                    span_copies(b * spans + c)[0].wait()
                    start_span(b * spans + c + 2)
                span_copies(b * spans + c)[1].wait()

        over = jnp.max(jnp.where(sum_ref[pl.ds(0, rows_all), :] < LIMIT, 0.0, 1.0))

        @pl.when(over > 0.0)
        def _():
            reset()

            def careful(rows, scores, values):
                old = m_ref[rows, :]
                level_up(rows, scores)
                shrink = jnp.exp2(old - m_ref[rows, :])
                mix_ref[rows, :] *= shrink
                sum_ref[rows, :] *= shrink
                add(rows, scores, values)

            @pl.when(last)
            def _():
                for r, rows in enumerate(halves):
                    careful(rows, draft_scores(b, r, rows), dv_ref[b])

            def step(t, carry):
                start = pl.multiple_of(t * TILE, TILE)

                @pl.when(start < left)
                def _():
                    for rows in halves:
                        careful(rows, tile_scores(b, rows, start, left), v_ref[b, pl.ds(start, TILE), :])

                return carry

            lax.fori_loop(0, local_span // TILE, step, 0)

        row = lax.broadcasted_iota(jnp.int32, (block_rows, LANES), 0)
        col = lax.broadcasted_iota(jnp.int32, (block_rows, LANES), 1)
        diagonal = jnp.logical_and(row == col, row < part)
        for d in range(count):
            rows = pl.ds(d * part, block_rows)
            total = sum_ref[rows, :]
            some = jnp.logical_and(row < part, total > 0.0)
            safe = jnp.where(some, total, 1.0)
            level = jnp.where(some, m_ref[rows, :] + jnp.log2(safe), masked_score)
            level = jnp.sum(jnp.where(diagonal, level, 0.0), axis=0, keepdims=True)
            high = level.astype(jnp.bfloat16).astype(jnp.float32)
            rest = level - high
            mid = rest.astype(jnp.bfloat16).astype(jnp.float32)
            low = rest - mid
            block = jnp.where(row < part, mix_ref[rows, :] / safe, 0.0)
            block = jnp.where(row == part, high, block)
            block = jnp.where(row == part + 1, mid, block)
            block = jnp.where(row == part + 2, low, block)
            out_ref[d, pl.ds(pl.multiple_of(b * block_rows, 8), block_rows), :] = block.astype(jnp.bfloat16)
        return carry

    lax.fori_loop(0, batch, one_request, 0)


def attend(lengths, place, q, keys, values, draft_keys, draft_values, kv_count, part, block_rows):
    batch, rows_all, width = q.shape
    local_span, draft = keys.shape[1], draft_keys.shape[1]
    span = math.gcd(local_span, 4096)
    kernel = functools.partial(
        attend_kernel, factor=math.log2(math.e) / math.sqrt(width), kv_count=kv_count,
        span=span, part=part, block_rows=block_rows,
    )
    anywhere = pl.BlockSpec(memory_space=pltpu.HBM)
    state = pltpu.VMEM((rows_all + block_rows, LANES), jnp.float32)
    out = (rows_all // part, batch * block_rows, width)
    return pl.pallas_call(
        kernel,
        out_shape=jax.ShapeDtypeStruct(out, jnp.bfloat16),
        grid_spec=pltpu.PrefetchScalarGridSpec(
            num_scalar_prefetch=1,
            grid=(1,),
            in_specs=[anywhere] * 6,
            out_specs=pl.BlockSpec(out, lambda i, *_: (0, 0, 0)),
            scratch_shapes=[
                pltpu.SMEM((batch,), jnp.int32),
                pltpu.VMEM((batch, rows_all, width), jnp.bfloat16),
                pltpu.VMEM((batch, local_span, width), jnp.bfloat16),
                pltpu.VMEM((batch, local_span, width), jnp.bfloat16),
                pltpu.VMEM((batch, draft, width), jnp.bfloat16),
                pltpu.VMEM((batch, draft, width), jnp.bfloat16),
                pltpu.VMEM((local_span, LANES), jnp.bfloat16),
                state, state, state,
                pltpu.SemaphoreType.DMA((2, batch * local_span // span)),
                pltpu.SemaphoreType.DMA((4,)),
            ],
        ),
        compiler_params=pltpu.CompilerParams(vmem_limit_bytes=58 * 2**20),
        cost_estimate=pl.CostEstimate(
            flops=4 * batch * rows_all * local_span * width,
            bytes_accessed=4 * batch * local_span * width,
            transcendentals=batch * rows_all * local_span,
        ),
        name="attend",
    )(place, lengths, q, keys, values, draft_keys, draft_values)


def merge_kernel(got_ref, out_ref, both_ref, *, part, batch):
    count, rows, width = got_ref.shape
    block_rows = rows // batch
    base = (part // 8) * 8
    at = part - base
    for b in range(batch):
        stats = got_ref[:, pl.ds(b * block_rows + base, block_rows - base), :].astype(jnp.float32)
        level = stats[:, at, :] + stats[:, at + 1, :] + stats[:, at + 2, :]
        share = jnp.exp2(level - jnp.max(level, axis=0, keepdims=True))
        share = share / jnp.sum(share, axis=0, keepdims=True)
        share = share.T
        total = jnp.zeros((block_rows, width), jnp.float32)
        for s in range(count):
            mine = got_ref[s, pl.ds(b * block_rows, block_rows), :].astype(jnp.float32)
            total = total + share[:block_rows, s : s + 1] * mine
        both_ref[pl.ds(b * part, block_rows), :] = total
    done = both_ref[pl.ds(0, batch * part), :].astype(out_ref.dtype)
    for s in range(count):
        out_ref[s] = done


def merge(got, part, batch):
    count, rows, width = got.shape
    return pl.pallas_call(
        functools.partial(merge_kernel, part=part, batch=batch),
        out_shape=jax.ShapeDtypeStruct((count, batch * part, width), jnp.bfloat16),
        scratch_shapes=[pltpu.VMEM((rows, width), jnp.float32)],
        compiler_params=pltpu.CompilerParams(vmem_limit_bytes=8 * 2**20),
        name="merge",
    )(got)


def project_kernel(a_ref, w_ref, out_ref, rows_ref, *, group, heads, batch):
    count, both, width = a_ref.shape
    part = both // batch
    draft = count * part // group
    cycle = math.lcm(group, part)
    steps = count * part // cycle
    half = width // 2
    for d in range(count):
        rows_ref[pl.ds(d * both, both), :] = a_ref[d].astype(jnp.float32)
    rows = []
    for b in range(batch):
        for j in range(cycle // group):
            line = []
            for g in range(group):
                d, r = divmod(j * group + g, part)
                at = pl.ds(d * both + b * part + r, steps, stride=cycle * batch)
                line.append(rows_ref[at, :])
            rows.append(jnp.concatenate(line, axis=1))
    rows = jnp.concatenate(rows, axis=0).astype(jnp.bfloat16)
    product = jnp.dot(rows, w_ref[...], preferred_element_type=jnp.float32)
    lane = lax.broadcasted_iota(jnp.int32, (draft, width), 1)
    for c in range(heads // 2):
        one = product[:draft, c * width : (c + 1) * width]
        two = product[draft:, c * width : (c + 1) * width]
        out_ref[2 * c] = jnp.where(lane < half, one, pltpu.roll(two, half, 1)).astype(out_ref.dtype)
        out_ref[2 * c + 1] = jnp.where(lane < half, pltpu.roll(one, half, 1), two).astype(out_ref.dtype)


def per_device(query, key_cache, value_cache, draft_keys, draft_values, lengths, out_weight):
    batch, draft, group, width = query.shape
    kv_count = lax.axis_size("kv")
    heads = lax.axis_size("head")
    local_span = key_cache.shape[2]
    part = draft * group // kv_count
    block_rows = -(-(part + 3) // 8) * 8
    place = lax.axis_index("kv").astype(jnp.int32)[None]
    exchange = functools.partial(lax.all_to_all, split_axis=0, concat_axis=0, tiled=True)
    sent = attend(
        lengths, place,
        query.reshape(batch, draft * group, width),
        key_cache.reshape(batch, local_span, width),
        value_cache.reshape(batch, local_span, width),
        draft_keys.reshape(batch, draft, width),
        draft_values.reshape(batch, draft, width),
        kv_count, part, block_rows,
    )
    everyone = exchange(merge(exchange(sent, "kv"), part, batch), "kv")
    shares = pl.pallas_call(
        functools.partial(project_kernel, group=group, heads=heads, batch=batch),
        out_shape=jax.ShapeDtypeStruct((heads, draft, width), jnp.bfloat16),
        scratch_shapes=[pltpu.VMEM((kv_count * batch * part, width), jnp.float32)],
        compiler_params=pltpu.CompilerParams(vmem_limit_bytes=16 * 2**20),
        name="project",
    )(everyone, out_weight)
    arrived = exchange(shares, "head")
    cycle = math.lcm(group, part) // group
    mixed = jnp.sum(arrived.astype(jnp.float32), axis=0)
    mixed = mixed.reshape(cycle, draft // cycle, batch, width // 2)
    mixed = jnp.transpose(mixed, (2, 1, 0, 3)).reshape(batch, draft, width // 2)
    return mixed.astype(jnp.bfloat16)


def solution(mesh):
    in_specs = (
        P(None, None, "head", None),
        P(None, "head", "kv", None),
        P(None, "head", "kv", None),
        P(None, "head", None, None),
        P(None, "head", None, None),
        P(),
        P("head", "kv"),
    )
    out_specs = P(None, None, ("kv", "head"))
    return jax.shard_map(
        per_device, mesh=mesh, in_specs=in_specs, out_specs=out_specs, check_vma=False
    )
```

```python
import functools
import math

import jax
import jax.numpy as jnp
from jax import lax
from jax.experimental import pallas as pl
from jax.experimental.pallas import tpu as pltpu
from jax.sharding import PartitionSpec as P

masked_score = -1e30
LANES = 128
TILE = 256
LIMIT = 2.0**120


def pair_scores(q, keys):
    return lax.dot_general(q, keys, (((1,), (1,)), ((), ())), preferred_element_type=jnp.float32)


def attend_kernel(
    place_ref, lengths_hbm, q_hbm, k_hbm, v_hbm, dk_hbm, dv_hbm, out_ref,
    out_s, lengths_ref, q_ref, k_ref, v_ref, dk_ref, dv_ref, one_ref, m_ref, mix_ref, sum_ref, sems, small_sems, out_sems,
    *, factor, kv_count, span, part, block_rows,
):
    batch, rows_all, width = q_ref.shape
    local_span = k_ref.shape[1]
    draft = dk_ref.shape[1]
    group = rows_all // draft
    spans = local_span // span
    count = rows_all // part
    half_rows = rows_all
    kv_index = place_ref[0]
    last = kv_index == kv_count - 1
    halves = [pl.ds(r * half_rows, half_rows) for r in range(1)]

    def small_copies():
        pairs = ((q_hbm, q_ref), (lengths_hbm, lengths_ref), (dk_hbm, dk_ref), (dv_hbm, dv_ref))
        return [pltpu.make_async_copy(a, z, small_sems.at[n]) for n, (a, z) in enumerate(pairs)]

    def span_copies(s):
        b = s // spans
        at = pl.ds(pl.multiple_of((s - b * spans) * span, span), span)
        return (
            pltpu.make_async_copy(k_hbm.at[b, at, :], k_ref.at[b, at, :], sems.at[0, s]),
            pltpu.make_async_copy(v_hbm.at[b, at, :], v_ref.at[b, at, :], sems.at[1, s]),
        )

    def start_span(s):
        @pl.when(s < batch * spans)
        def _():
            for copy in span_copies(s):
                copy.start()

    for copy in small_copies()[:2]:
        copy.start()
    for copy in span_copies(0):
        copy.start()
    for copy in small_copies()[2:]:
        copy.start()
    one_ref[...] = jnp.ones(one_ref.shape, one_ref.dtype)
    for copy in small_copies():
        copy.wait()
    start_span(1)

    def reset():
        for ref, fill in ((mix_ref, 0.0), (sum_ref, 0.0), (m_ref, masked_score)):
            ref[pl.ds(0, rows_all), :] = jnp.full((rows_all, LANES), fill, jnp.float32)

    def draft_scores(b, r, rows):
        row = r * half_rows + lax.broadcasted_iota(jnp.int32, (half_rows, draft), 0)
        col = lax.broadcasted_iota(jnp.int32, (half_rows, draft), 1)
        scores = pair_scores(q_ref[b, rows, :], dk_ref[b]) * factor
        return jnp.where(col * group <= row, scores, masked_score)

    def tile_scores(b, rows, start, left):
        at = start + lax.broadcasted_iota(jnp.int32, (half_rows, TILE), 1)
        scores = pair_scores(q_ref[b, rows, :], k_ref[b, pl.ds(start, TILE), :]) * factor
        return jnp.where(at < left, scores, masked_score)

    def level_up(rows, scores):
        m_ref[rows, :] = jnp.maximum(m_ref[rows, :], jnp.max(scores, axis=1, keepdims=True))

    def add(rows, scores, values):
        weights = jnp.exp2(scores - m_ref[rows, :][:, :1]).astype(jnp.bfloat16)
        wide = jnp.concatenate([values, jnp.ones(values.shape, values.dtype)], axis=1)
        fresh = jnp.dot(weights, wide, preferred_element_type=jnp.float32)
        mix_ref[rows, :] += fresh[:, :LANES]
        sum_ref[rows, :] += fresh[:, LANES:]

    def ready(b, c, left):
        s = b * spans + c
        if c > 0:
            span_copies(s)[0].wait()
            start_span(s + 2)
        span_copies(s)[1].wait()
        rest = left - c * span

        @pl.when(rest < span)
        def _():
            def cut(t, carry):
                here = pl.ds(pl.multiple_of(c * span + t * TILE, TILE), TILE)
                at = t * TILE + lax.broadcasted_iota(jnp.int32, (TILE, width), 0)
                keep = at < rest
                kept = jnp.where(keep, v_ref[b, here, :].astype(jnp.float32), 0.0)
                v_ref[b, here, :] = kept.astype(v_ref.dtype)
                one_ref[here, :] = jnp.where(keep, 1.0, 0.0).astype(one_ref.dtype)
                return carry

            lax.fori_loop(0, span // TILE, cut, 0)

    def sweep(b, left):
        for r, rows in enumerate(halves):
            q = q_ref[b, rows, :]
            level = m_ref[rows, :]
            level = jnp.concatenate([level, level], axis=1)
            total = jnp.zeros((half_rows, 2 * LANES), jnp.float32)
            for t in range(local_span // TILE):
                if r == 0 and t * TILE % span == 0:
                    ready(b, t * TILE // span, left)
                at = pl.ds(t * TILE, TILE)
                scores = pair_scores(q, k_ref[b, at, :]) * factor
                weights = jnp.exp2(scores - level).astype(jnp.bfloat16)
                wide = jnp.concatenate([v_ref[b, at, :], one_ref[at, :]], axis=1)
                total += jnp.dot(weights, wide, preferred_element_type=jnp.float32)
            mix_ref[rows, :] += total[:, :LANES]
            sum_ref[rows, :] += total[:, LANES:]

    def one_request(b, carry):
        left = lengths_ref[b] - kv_index * local_span
        reset()

        @pl.when(last)
        def _():
            for r, rows in enumerate(halves):
                level_up(rows, draft_scores(b, r, rows))

        span_copies(b * spans)[0].wait()
        start_span(b * spans + 2)

        @pl.when(left > 0)
        def _():
            for rows in halves:
                level_up(rows, tile_scores(b, rows, 0, left))

        @pl.when(last)
        def _():
            for r, rows in enumerate(halves):
                add(rows, draft_scores(b, r, rows), dv_ref[b])

        @pl.when(left > 0)
        def _():
            sweep(b, left)

            @pl.when(left < local_span)
            def _():
                one_ref[...] = jnp.ones(one_ref.shape, one_ref.dtype)

        @pl.when(left <= 0)
        def _():
            for c in range(spans):
                if c > 0:
                    span_copies(b * spans + c)[0].wait()
                    start_span(b * spans + c + 2)
                span_copies(b * spans + c)[1].wait()

        over = jnp.max(jnp.where(sum_ref[pl.ds(0, rows_all), :] < LIMIT, 0.0, 1.0))

        @pl.when(over > 0.0)
        def _():
            reset()

            def careful(rows, scores, values):
                old = m_ref[rows, :]
                level_up(rows, scores)
                shrink = jnp.exp2(old - m_ref[rows, :])
                mix_ref[rows, :] *= shrink
                sum_ref[rows, :] *= shrink
                add(rows, scores, values)

            @pl.when(last)
            def _():
                for r, rows in enumerate(halves):
                    careful(rows, draft_scores(b, r, rows), dv_ref[b])

            def step(t, carry):
                start = pl.multiple_of(t * TILE, TILE)

                @pl.when(start < left)
                def _():
                    for rows in halves:
                        careful(rows, tile_scores(b, rows, start, left), v_ref[b, pl.ds(start, TILE), :])

                return carry

            lax.fori_loop(0, local_span // TILE, step, 0)

        row = lax.broadcasted_iota(jnp.int32, (block_rows, LANES), 0)
        col = lax.broadcasted_iota(jnp.int32, (block_rows, LANES), 1)
        diagonal = jnp.logical_and(row == col, row < part)
        for d in range(count):
            rows = pl.ds(d * part, block_rows)
            total = sum_ref[rows, :]
            some = jnp.logical_and(row < part, total > 0.0)
            safe = jnp.where(some, total, 1.0)
            level = jnp.where(some, m_ref[rows, :] + jnp.log2(safe), masked_score)
            level = jnp.sum(jnp.where(diagonal, level, 0.0), axis=0, keepdims=True)
            high = level.astype(jnp.bfloat16).astype(jnp.float32)
            rest = level - high
            mid = rest.astype(jnp.bfloat16).astype(jnp.float32)
            low = rest - mid
            block = jnp.where(row < part, mix_ref[rows, :] / safe, 0.0)
            block = jnp.where(row == part, high, block)
            block = jnp.where(row == part + 1, mid, block)
            block = jnp.where(row == part + 2, low, block)
            out_s[b, d] = block.astype(jnp.bfloat16)
        out_copy(b).start()
        return carry

    def out_copy(b):
        there = pl.ds(pl.multiple_of(b * block_rows, 8), block_rows)
        return pltpu.make_async_copy(out_s.at[b], out_ref.at[:, there, :], out_sems.at[b])

    lax.fori_loop(0, batch, one_request, 0)
    for b in range(batch):
        out_copy(b).wait()


def attend(lengths, place, q, keys, values, draft_keys, draft_values, kv_count, part, block_rows):
    batch, rows_all, width = q.shape
    local_span, draft = keys.shape[1], draft_keys.shape[1]
    span = math.gcd(local_span, 4096)
    kernel = functools.partial(
        attend_kernel, factor=math.log2(math.e) / math.sqrt(width), kv_count=kv_count,
        span=span, part=part, block_rows=block_rows,
    )
    anywhere = pl.BlockSpec(memory_space=pltpu.HBM)
    state = pltpu.VMEM((rows_all + block_rows, LANES), jnp.float32)
    out = (rows_all // part, batch * block_rows, width)
    return pl.pallas_call(
        kernel,
        out_shape=jax.ShapeDtypeStruct(out, jnp.bfloat16),
        grid_spec=pltpu.PrefetchScalarGridSpec(
            num_scalar_prefetch=1,
            grid=(1,),
            in_specs=[anywhere] * 6,
            out_specs=anywhere,
            scratch_shapes=[
                pltpu.VMEM((batch, rows_all // part, block_rows, width), jnp.bfloat16),
                pltpu.SMEM((batch,), jnp.int32),
                pltpu.VMEM((batch, rows_all, width), jnp.bfloat16),
                pltpu.VMEM((batch, local_span, width), jnp.bfloat16),
                pltpu.VMEM((batch, local_span, width), jnp.bfloat16),
                pltpu.VMEM((batch, draft, width), jnp.bfloat16),
                pltpu.VMEM((batch, draft, width), jnp.bfloat16),
                pltpu.VMEM((local_span, LANES), jnp.bfloat16),
                state, state, state,
                pltpu.SemaphoreType.DMA((2, batch * local_span // span)),
                pltpu.SemaphoreType.DMA((4,)),
                pltpu.SemaphoreType.DMA((batch,)),
            ],
        ),
        compiler_params=pltpu.CompilerParams(vmem_limit_bytes=58 * 2**20),
        cost_estimate=pl.CostEstimate(
            flops=4 * batch * rows_all * local_span * width,
            bytes_accessed=4 * batch * local_span * width,
            transcendentals=batch * rows_all * local_span,
        ),
        name="attend",
    )(place, lengths, q, keys, values, draft_keys, draft_values)


def merge_kernel(got_ref, out_ref, both_ref, *, part, batch):
    count, rows, width = got_ref.shape
    block_rows = rows // batch
    base = (part // 8) * 8
    at = part - base
    for b in range(batch):
        stats = got_ref[:, pl.ds(b * block_rows + base, block_rows - base), :].astype(jnp.float32)
        level = stats[:, at, :] + stats[:, at + 1, :] + stats[:, at + 2, :]
        share = jnp.exp2(level - jnp.max(level, axis=0, keepdims=True))
        share = share / jnp.sum(share, axis=0, keepdims=True)
        share = share.T
        total = jnp.zeros((block_rows, width), jnp.float32)
        for s in range(count):
            mine = got_ref[s, pl.ds(b * block_rows, block_rows), :].astype(jnp.float32)
            total = total + share[:block_rows, s : s + 1] * mine
        both_ref[pl.ds(b * part, block_rows), :] = total
    done = both_ref[pl.ds(0, batch * part), :].astype(out_ref.dtype)
    for s in range(count):
        out_ref[s] = done


def merge(got, part, batch):
    count, rows, width = got.shape
    return pl.pallas_call(
        functools.partial(merge_kernel, part=part, batch=batch),
        out_shape=jax.ShapeDtypeStruct((count, batch * part, width), jnp.bfloat16),
        scratch_shapes=[pltpu.VMEM((rows, width), jnp.float32)],
        compiler_params=pltpu.CompilerParams(vmem_limit_bytes=8 * 2**20),
        name="merge",
    )(got)


def project_kernel(a_ref, w_ref, out_ref, rows_ref, *, group, heads, batch):
    count, both, width = a_ref.shape
    part = both // batch
    draft = count * part // group
    cycle = math.lcm(group, part)
    steps = count * part // cycle
    half = width // 2
    for d in range(count):
        rows_ref[pl.ds(d * both, both), :] = a_ref[d].astype(jnp.float32)
    rows = []
    for b in range(batch):
        for j in range(cycle // group):
            line = []
            for g in range(group):
                d, r = divmod(j * group + g, part)
                at = pl.ds(d * both + b * part + r, steps, stride=cycle * batch)
                line.append(rows_ref[at, :])
            rows.append(jnp.concatenate(line, axis=1))
    rows = jnp.concatenate(rows, axis=0).astype(jnp.bfloat16)
    product = jnp.dot(rows, w_ref[...], preferred_element_type=jnp.float32)
    lane = lax.broadcasted_iota(jnp.int32, (draft, width), 1)
    for c in range(heads // 2):
        one = product[:draft, c * width : (c + 1) * width]
        two = product[draft:, c * width : (c + 1) * width]
        out_ref[2 * c] = jnp.where(lane < half, one, pltpu.roll(two, half, 1)).astype(out_ref.dtype)
        out_ref[2 * c + 1] = jnp.where(lane < half, pltpu.roll(one, half, 1), two).astype(out_ref.dtype)


def per_device(query, key_cache, value_cache, draft_keys, draft_values, lengths, out_weight):
    batch, draft, group, width = query.shape
    kv_count = lax.axis_size("kv")
    heads = lax.axis_size("head")
    local_span = key_cache.shape[2]
    part = draft * group // kv_count
    block_rows = -(-(part + 3) // 8) * 8
    place = lax.axis_index("kv").astype(jnp.int32)[None]
    exchange = functools.partial(lax.all_to_all, split_axis=0, concat_axis=0, tiled=True)
    sent = attend(
        lengths, place,
        query.reshape(batch, draft * group, width),
        key_cache.reshape(batch, local_span, width),
        value_cache.reshape(batch, local_span, width),
        draft_keys.reshape(batch, draft, width),
        draft_values.reshape(batch, draft, width),
        kv_count, part, block_rows,
    )
    everyone = exchange(merge(exchange(sent, "kv"), part, batch), "kv")
    shares = pl.pallas_call(
        functools.partial(project_kernel, group=group, heads=heads, batch=batch),
        out_shape=jax.ShapeDtypeStruct((heads, draft, width), jnp.bfloat16),
        scratch_shapes=[pltpu.VMEM((kv_count * batch * part, width), jnp.float32)],
        compiler_params=pltpu.CompilerParams(vmem_limit_bytes=16 * 2**20),
        name="project",
    )(everyone, out_weight)
    arrived = exchange(shares, "head")
    cycle = math.lcm(group, part) // group
    mixed = jnp.sum(arrived.astype(jnp.float32), axis=0)
    mixed = mixed.reshape(cycle, draft // cycle, batch, width // 2)
    mixed = jnp.transpose(mixed, (2, 1, 0, 3)).reshape(batch, draft, width // 2)
    return mixed.astype(jnp.bfloat16)


def solution(mesh):
    in_specs = (
        P(None, None, "head", None),
        P(None, "head", "kv", None),
        P(None, "head", "kv", None),
        P(None, "head", None, None),
        P(None, "head", None, None),
        P(),
        P("head", "kv"),
    )
    out_specs = P(None, None, ("kv", "head"))
    return jax.shard_map(
        per_device, mesh=mesh, in_specs=in_specs, out_specs=out_specs, check_vma=False
    )
```
